32 devices in a mesh: sub: 8 (over z, y), split: 4 (over x, core).
Axes of the slice: x: 2, y: 2, z: 4, core: 2. Of those that a mesh axis runs over, the one named last changes fastest.
Arguments:
- inv_conductance: float32 [8, 2048, 2048], P('sub', None, 'split')
- source_amp: float32 [8, 2048], P('sub', 'split'), may hold values from -6 to 6
- source_phase: float32 [8, 2048], P('sub', 'split'), may hold values from -3.140625 to 3.140625
- companion: float32 [8, 2048], P('sub', 'split'), may hold values from 0.1 to 0.8
- surge_impedance: float32 [8, 512], P('sub', 'split'), may hold values from 2 to 8
- initial_voltage: float32 [8, 64, 2048], P('sub', None, 'split'), may hold values from -6 to 6
- initial_history: float32 [8, 64, 512], P('sub', None, 'split'), may hold values from -6 to 6
- partner_sub: int32 [8, 512], P('sub', 'split'), may hold values from 0 to 7, as said below
- line_delay: int32 [8, 512], P('sub', 'split'), may hold values from 2 to 5, as said below
- open_step: int32 [8, 64, 512], P('sub', None, 'split'), may hold values from 0 to 15
Outputs:
- voltage: float32 [8, 64, 2048], P('sub', None, 'split')
- port_current: float32 [8, 64, 512], P('sub', None, 'split')
The draws below stay inside these ranges and needn't reach their ends.
Inputs may be any that keep to these rules, and one draw needn't show every extreme that they name: partner_sub[partner_sub[s, p], p] == s and partner_sub[s, p] != s: a line joins port p of two subnetworks, both in the same block of 128 ports. At most 32 ports of one block of a subnetwork have lines to the same other subnetwork, and in every block some subnetwork gets exactly 32. `line_delay`: both ends of a line have the same delay.
All inputs are finite; a program needn't handle non-finite values.
Results may differ from the reference program's by a relative error of at most 0.00015.
Values sent between devices are 32-bit elements; how exact they have to be, the bound alone decides.
A program may use at most 64 MiB of HBM per device.

```python
import math
import jax
import jax.numpy as jnp
from jax import lax

NODES = 2048
PORTS = 512
CONT = 64
STEPS = 8
DMIN = 2
DMAX = 5
SUBS = 8
PORTS_DEV = 128
CAP = 32


def draw_inv_conductance(key, part):
    first, second = jax.random.split(jax.random.fold_in(key, 17))
    diagonal = jax.random.uniform(first, (SUBS, NODES), jnp.float32, 0.3, 0.9)
    spread = jax.random.normal(second, (SUBS, NODES, NODES), jnp.float32) * (0.3 / NODES ** 0.5)
    return spread + diagonal[:, :, None] * jnp.eye(NODES, dtype=jnp.float32)[None]


def line_block(block_key):
    keys = jax.random.split(block_key, 5)
    order = jax.random.permutation(keys[0], PORTS_DEV).astype(jnp.int32)
    relabel = jax.random.permutation(keys[1], SUBS).astype(jnp.int32)
    inverse = jnp.argsort(relabel).astype(jnp.int32)
    offset = jax.random.randint(keys[2], (), 0, SUBS - 1)
    group = order // CAP
    flip = 1 + (group + offset) % (SUBS - 1)
    label = relabel[:, None]
    other = jnp.bitwise_xor(label, flip[None, :])
    partner = inverse[other]
    lower = jnp.minimum(label, other)
    delay_table = jax.random.randint(keys[4], (SUBS, PORTS_DEV), DMIN, DMAX + 1)
    delay = delay_table[lower, order[None, :]]
    return (partner.astype(jnp.int32), delay.astype(jnp.int32))


def line_tables(key):
    blocks = [line_block(jax.random.fold_in(key, 1000 + number)) for number in range(PORTS // PORTS_DEV)]
    return tuple((jnp.concatenate([entry[which] for entry in blocks], 1) for which in range(2)))


def draw_partner_sub(key, part):
    return line_tables(key)[0]


def draw_line_delay(key, part):
    return line_tables(key)[1]


def with_ends(drawn, stream_key, low, largest):
    place = [jax.random.randint(jax.random.fold_in(stream_key, axis), (), 0, length) for axis, length in enumerate(drawn.shape)]
    widest = drawn.shape.index(max(drawn.shape))
    next_to = place[:widest] + [(place[widest] + 1) % drawn.shape[widest]] + place[widest + 1:]
    return drawn.at[tuple(place)].set(low).at[tuple(next_to)].set(largest)


def level_of(key, extent, pieces, least, top_value):
    factor_of = 1.0
    for dim, parts in pieces:
        steps = jax.random.uniform(jax.random.fold_in(jax.random.fold_in(key, 6), dim), (parts,), jnp.float32, least / len(pieces), top_value / len(pieces))
        factor_of = factor_of * jnp.repeat(jnp.exp(steps), extent[dim] // parts).reshape((-1,) + (1,) * (len(extent) - 1 - dim))
    return factor_of


def gaussian(rng, shape, scale, bound, shards=(), kind=jnp.bfloat16):
    gain = level_of(rng, shape, shards, -0.22, 0.18) if shards else 1.0
    drawn = jax.random.normal(rng, shape, jnp.float32) * scale * gain
    return jnp.minimum(jnp.maximum(drawn, -bound), bound).astype(kind)


def setup_inputs(seed: int = 0) -> dict:
    streams_of = jax.random.split(jax.random.key(seed), 11)
    inv_conductance = draw_inv_conductance(jax.random.fold_in(streams_of[10], 71), 0)
    source_amp = gaussian(streams_of[1], (SUBS, NODES), 1.0, 6.0, ((0, 8), (1, 4)), jnp.float32)
    source_phase = jnp.clip(jax.random.uniform(streams_of[2], (SUBS, NODES), jnp.float32, -3.140625, 3.140625), -3.140625, 3.140625)
    companion = jnp.clip(jnp.exp(math.log(0.8) - 2.0794415 * jax.random.uniform(streams_of[3], (SUBS, NODES), jnp.float32) ** level_of(streams_of[3], (SUBS, NODES), ((0, 8), (1, 4)), -0.2, 0.2)), 0.1, 0.8)
    surge_impedance = jnp.clip(jnp.exp(math.log(8.0) - 1.3862944 * jax.random.uniform(streams_of[4], (SUBS, PORTS), jnp.float32) ** level_of(streams_of[4], (SUBS, PORTS), ((0, 8), (1, 4)), -0.2, 0.2)), 2.0, 8.0)
    initial_voltage = gaussian(streams_of[5], (SUBS, CONT, NODES), 1.0, 6.0, ((0, 8), (2, 4)), jnp.float32)
    initial_history = gaussian(streams_of[6], (SUBS, CONT, PORTS), 1.0, 6.0, ((0, 8), (2, 4)), jnp.float32)
    partner_sub = draw_partner_sub(jax.random.fold_in(streams_of[10], 71), 0)
    line_delay = draw_line_delay(jax.random.fold_in(streams_of[10], 71), 0)
    open_step = with_ends(jax.random.randint(streams_of[9], (SUBS, CONT, PORTS), 0, 2 * STEPS), jax.random.fold_in(streams_of[9], 1), 0, (2 * STEPS) - 1).astype(jnp.int32)
    return {"inv_conductance": inv_conductance, "source_amp": source_amp, "source_phase": source_phase, "companion": companion, "surge_impedance": surge_impedance, "initial_voltage": initial_voltage, "initial_history": initial_history, "partner_sub": partner_sub, "line_delay": line_delay, "open_step": open_step}


angular = 0.7


def reference(inv_conductance, source_amp, source_phase, companion, surge_impedance, initial_voltage, initial_history, partner_sub, line_delay, open_step):
    subs = inv_conductance.shape[0]
    cont = initial_voltage.shape[1]
    ports = initial_history.shape[2]
    stride = NODES // PORTS
    voltage = initial_voltage
    delays = line_delay[:, None, :]
    index = jnp.broadcast_to(partner_sub[:, None, :], (subs, cont, ports)).astype(jnp.int32)
    arrived = []
    current = jnp.zeros_like(initial_history)
    for step in range(STEPS):
        closed = (step < open_step).astype(jnp.float32)
        history = jnp.where(step < delays, initial_history, jnp.float32(0.0))
        for anchor, outgoing in enumerate(arrived):
            far_end = jnp.take_along_axis(outgoing, index, axis=0)
            history = jnp.where(delays == step - anchor, -far_end, history)
        inject = closed * history
        spread = jnp.concatenate([inject[:, :, :, None], jnp.zeros((subs, cont, ports, stride - 1), jnp.float32)], 3).reshape(subs, cont, NODES)
        source = source_amp * jnp.cos(angular * (step + 1) + source_phase)
        right_side = source[:, None, :] + companion[:, None, :] * voltage - spread
        voltage = jnp.einsum("scm,snm->scn", right_side, inv_conductance, precision=lax.Precision.HIGHEST)
        at_ports = voltage.reshape(subs, cont, ports, stride)[:, :, :, 0]
        impedance = surge_impedance[:, None, :]
        arrived.append(closed * (2.0 * at_ports / impedance + history))
        current = closed * (at_ports / impedance + history)
    return voltage, current
```

```python
import functools

import jax
import jax.numpy as jnp
from jax import lax
from jax.experimental import pallas as pl
from jax.experimental.pallas import tpu as pltpu
from jax.sharding import PartitionSpec as P

STEPS = 8
DMIN = 2
DMAX = 5
HALVES = 2
MESH = pl.DeviceIdType.MESH

angular = 0.7
NT = (((1,), (1,)), ((), ()))
NN = (((1,), (0,)), ((), ()))


def dot(a, b, dims=NN):
    return lax.dot_general(a, b, dims, preferred_element_type=jnp.float32)


def parts_of(x, count):
    terms = []
    for _ in range(count):
        term = x.astype(jnp.bfloat16)
        terms.append(term)
        x = x - term.astype(jnp.float32)
    return terms


def exact_dot(x, onehot, dims):
    rows = x.shape[0]
    stacked = dot(jnp.concatenate(parts_of(x, 3), 0), onehot, dims)
    return (stacked[:rows] + stacked[rows : 2 * rows]) + stacked[2 * rows :]


def kernel(
    n_subs,
    inv_ref,
    amp_ref,
    phase_ref,
    comp_ref,
    surge_ref,
    volt_ref,
    hist0_ref,
    partner_ref,
    delay_ref,
    open_ref,
    out_volt_ref,
    out_cur_ref,
    mat,
    high,
    low,
    perm,
    vol,
    src,
    kept,
    outg,
    hist,
    far,
    send_a,
    send_b,
    send_c,
    recv_a,
    recv_b,
    recv_c,
    port_recv,
    load_sem,
    sems,
    psend,
    precv,
):
    sub = lax.axis_index("sub")
    me = lax.axis_index("split")
    sibling = me + 1 - 2 * lax.rem(me, 2)
    across = lax.rem(me + 2, 4)
    diagonal = lax.rem(sibling + 2, 4)
    cont = volt_ref.shape[1]
    nodes = volt_ref.shape[2]
    ports = hist0_ref.shape[2]
    stride = nodes // ports
    rows = cont // HALVES
    owners = (diagonal, across, sibling, me)

    strips = nodes // 128

    def load(slot, i):
        start = pl.multiple_of(owners[slot] * nodes, nodes)
        return pltpu.make_async_copy(
            inv_ref.at[0, pl.ds(start, nodes), pl.ds(i * 128, 128)],
            mat.at[i, pl.ds(slot * nodes, nodes), :],
            load_sem.at[slot, i],
        )

    for slot in range(4):
        for i in range(strips):
            load(slot, i).start()

    barrier = pltpu.get_barrier_semaphore()
    for other in (sibling, across):
        pl.semaphore_signal(barrier, inc=1, device_id=(sub, other), device_id_type=MESH)

    def each_peer(body):
        if n_subs <= 16:
            for j in range(1, n_subs):
                body(j)
        else:

            def step_of(j, c):
                body(j)
                return c

            lax.fori_loop(1, n_subs, step_of, 0)

    def greet(j):
        pl.semaphore_signal(
            barrier, inc=1, device_id=(lax.rem(sub + j, n_subs), me), device_id_type=MESH
        )

    each_peer(greet)

    line = lax.broadcasted_iota(jnp.int32, (nodes, nodes), 0)
    node = lax.broadcasted_iota(jnp.int32, (nodes, nodes), 1)
    wanted = (line % ports) * stride + line // ports
    perm[...] = jnp.where(node == wanted, 1.0, 0.0).astype(jnp.bfloat16)

    small = jnp.concatenate(
        [amp_ref[...], phase_ref[...], comp_ref[...], jnp.zeros((5, nodes), jnp.float32), volt_ref[0]], 0
    )
    small = exact_dot(small, perm[...], NT)
    amp, phase = small[0:1], small[1:2]
    when = (lax.broadcasted_iota(jnp.int32, (STEPS, nodes), 0) + 1).astype(jnp.float32)
    source = amp * jnp.cos(jnp.float32(angular) * when + phase)
    for step in range(STEPS):
        src[step] = source[step : step + 1]
    src[STEPS] = small[2:3]
    for half in range(HALVES):
        vol[half] = small[8 + half * rows : 8 + (half + 1) * rows]
        for early in range(DMAX):
            far[early, half] = -hist0_ref[0, half * rows : (half + 1) * rows, :]

    def prepare(slot, c):
        base = pl.multiple_of(slot * nodes, nodes)
        for j in range(stride):
            chunk = jnp.concatenate(
                [
                    mat[i, pl.ds(base + j, ports, stride=stride), :]
                    for i in range(strips)
                ],
                1,
            )
            top, rest = parts_of(chunk, 2)
            cols = pl.ds(j * ports, ports)
            high[slot, :, cols] = dot(perm[...], top, NT).astype(jnp.bfloat16)
            low[slot, :, cols] = dot(perm[...], rest, NT).astype(jnp.bfloat16)
        return c

    for slot in range(4):
        for i in range(strips):
            load(slot, i).wait()
    lax.fori_loop(0, 4, prepare, 0)

    pl.semaphore_wait(barrier, n_subs + 1)

    def remote(kind, t, half):
        source_ref, target_ref, device = (
            (send_a, recv_a, sibling),
            (send_b, recv_b, sibling),
            (send_c, recv_c, across),
        )[kind]
        return pltpu.make_async_remote_copy(
            src_ref=source_ref.at[t, half],
            dst_ref=target_ref.at[t, half],
            send_sem=sems.at[0, kind, t, half],
            recv_sem=sems.at[1, kind, t, half],
            device_id=(sub, device),
            device_id_type=MESH,
        )

    impedance = surge_ref[...]
    partner = partner_ref[...]
    delays = delay_ref[...]

    def all_ports(t, half, sem):
        return pltpu.make_async_copy(port_recv.at[t, half], port_recv.at[t, half], sem.at[t, half])

    def opened(t, half):
        return t < open_ref[0, half * rows : (half + 1) * rows, :]

    def finish(t, half):
        remote(1, t, half).wait_recv()
        remote(2, t, half).wait_recv()
        done = kept[half] + recv_b[t, half] + recv_c[t, half]
        vol[half] = done
        return done

    def ports_out(t, half, done):
        ratio = done[:, :ports] / impedance
        value = jnp.where(opened(t, half), 2.0 * ratio + hist[half], 0.0)
        outg[t, half] = value

        def send(j):
            pltpu.make_async_remote_copy(
                src_ref=outg.at[t, half],
                dst_ref=port_recv.at[t, half, j - 1],
                send_sem=psend.at[t, half],
                recv_sem=precv.at[t, half],
                device_id=(lax.rem(sub + j, n_subs), me),
                device_id_type=MESH,
            ).start()

        each_peer(send)

    def ports_in(t, half):
        all_ports(t, half, precv).wait()

        def pick(j, total):
            origin = lax.rem(sub + n_subs - j, n_subs)
            return jnp.where(partner == origin, port_recv[t, half, j - 1], total)

        total = jnp.zeros((rows, ports), jnp.float32)
        if n_subs <= 16:
            for j in range(1, n_subs):
                total = pick(j, total)
        else:
            total = lax.fori_loop(1, n_subs, pick, total)
        far[t + DMAX, half] = total

    def step_of(t, c):
        for half in range(HALVES):

            @pl.when(t >= 1)
            def _():
                done = finish(t - 1, half)

                @pl.when(t - 1 + DMIN < STEPS)
                def _():
                    ports_out(t - 1, half, done)

            @pl.when(t >= DMIN)
            def _():
                ports_in(t - DMIN, half)

            history = jnp.zeros((rows, ports), jnp.float32)
            for d in range(DMIN, DMAX + 1):
                history = jnp.where(delays == d, -far[t - d + DMAX, half], history)
            hist[half] = history
            inject = jnp.where(opened(t, half), history, 0.0)
            right = src[t] + src[STEPS] * vol[half]
            right = jnp.concatenate([right[:, :ports] - inject, right[:, ports:]], 1)
            both = jnp.concatenate(parts_of(right, 2), 0)

            def product(slot):
                twice = dot(both, high[slot])
                return (twice[:rows] + twice[rows:]) + dot(both[:rows], low[slot])

            send_a[t, half] = product(0)
            remote(0, t, half).start()
            mine = product(1)
            send_b[t, half] = product(2)
            remote(1, t, half).start()
            kept[half] = product(3)
            remote(0, t, half).wait_recv()
            send_c[t, half] = mine + recv_a[t, half]
            remote(2, t, half).start()
        return c

    lax.fori_loop(0, STEPS, step_of, 0)

    last = STEPS - 1
    for half in range(HALVES):
        done = finish(last, half)
        span = slice(half * rows, (half + 1) * rows)
        ratio = done[:, :ports] / impedance
        out_cur_ref[0, span, :] = jnp.where(opened(last, half), ratio + hist[half], 0.0)
        out_volt_ref[0, span, :] = exact_dot(done, perm[...], NN)

    def drain(t, c):
        for half in range(HALVES):
            for kind in range(3):
                remote(kind, t, half).wait_send()

            @pl.when(t + DMIN < STEPS)
            def _():
                all_ports(t, half, psend).wait()

        return c

    lax.fori_loop(0, STEPS, drain, 0)


def local(*args):
    n_subs = lax.axis_size("sub")
    volt, hist0 = args[5], args[6]
    cont, nodes = volt.shape[1], volt.shape[2]
    ports = hist0.shape[2]
    rows = cont // HALVES
    f32, bf16 = jnp.float32, jnp.bfloat16
    block = (STEPS, HALVES, rows, nodes)
    vmem = pl.BlockSpec(memory_space=pltpu.VMEM)
    moves = STEPS - DMIN
    dma = pltpu.SemaphoreType.DMA
    return pl.pallas_call(
        functools.partial(kernel, n_subs),
        out_shape=(
            jax.ShapeDtypeStruct(volt.shape, f32),
            jax.ShapeDtypeStruct(hist0.shape, f32),
        ),
        in_specs=[pl.BlockSpec(memory_space=pl.ANY)] + [vmem] * 9,
        out_specs=(vmem, vmem),
        scratch_shapes=[
            pltpu.VMEM((nodes // 128, 4 * nodes, 128), f32),
            pltpu.VMEM((4, nodes, nodes), bf16),
            pltpu.VMEM((4, nodes, nodes), bf16),
            pltpu.VMEM((nodes, nodes), bf16),
            pltpu.VMEM((HALVES, rows, nodes), f32),
            pltpu.VMEM((STEPS + 1, 1, nodes), f32),
            pltpu.VMEM((HALVES, rows, nodes), f32),
            pltpu.VMEM((moves, HALVES, rows, ports), f32),
            pltpu.VMEM((HALVES, rows, ports), f32),
            pltpu.VMEM((STEPS + DMAX, HALVES, rows, ports), f32),
            pltpu.VMEM(block, f32),
            pltpu.VMEM(block, f32),
            pltpu.VMEM(block, f32),
            pltpu.VMEM(block, f32),
            pltpu.VMEM(block, f32),
            pltpu.VMEM(block, f32),
            pltpu.VMEM((moves, HALVES, n_subs - 1, rows, ports), f32),
            dma((4, nodes // 128)),
            dma((2, 3, STEPS, HALVES)),
            dma((moves, HALVES)),
            dma((moves, HALVES)),
        ],
        compiler_params=pltpu.CompilerParams(
            collective_id=0, has_side_effects=True, vmem_limit_bytes=62 * 1024 * 1024
        ),
    )(*args)


def solution(mesh):
    placed = (
        P("sub", None, "split"),
        P("sub", "split"),
        P("sub", "split"),
        P("sub", "split"),
        P("sub", "split"),
        P("sub", None, "split"),
        P("sub", None, "split"),
        P("sub", "split"),
        P("sub", "split"),
        P("sub", None, "split"),
    )
    return jax.shard_map(
        local,
        mesh=mesh,
        in_specs=placed,
        out_specs=(P("sub", None, "split"), P("sub", None, "split")),
        check_vma=False,
    )
```

```python
import functools

import jax
import jax.numpy as jnp
from jax import lax
from jax.experimental import pallas as pl
from jax.experimental.pallas import tpu as pltpu
from jax.sharding import PartitionSpec as P

STEPS = 8
DMIN = 2
DMAX = 5
HALVES = 2
GROUPS = 2
LAG = 0
MESH = pl.DeviceIdType.MESH

angular = 0.7
NT = (((1,), (1,)), ((), ()))
NN = (((1,), (0,)), ((), ()))


def dot(a, b, dims=NN):
    return lax.dot_general(a, b, dims, preferred_element_type=jnp.float32)


def parts_of(x, count):
    terms = []
    for _ in range(count):
        term = x.astype(jnp.bfloat16)
        terms.append(term)
        x = x - term.astype(jnp.float32)
    return terms


def packing(n_subs, ports, cont):
    capacity = max(2, 2 * ports // n_subs)
    lanes = ports // capacity
    fits = n_subs * ports <= 1024 and (cont // GROUPS) % (8 * lanes) == 0
    return fits and ports % capacity == 0, capacity, lanes


def exact_dot(x, onehot, dims):
    rows = x.shape[0]
    stacked = dot(jnp.concatenate(parts_of(x, 3), 0), onehot, dims)
    return (stacked[:rows] + stacked[rows : 2 * rows]) + stacked[2 * rows :]


def kernel(
    n_subs,
    inv_ref,
    amp_ref,
    phase_ref,
    comp_ref,
    surge_ref,
    volt_ref,
    hist0_ref,
    partner_ref,
    delay_ref,
    open_ref,
    out_volt_ref,
    out_cur_ref,
    mat,
    high,
    low,
    perm,
    vol,
    src,
    kept,
    mine,
    value,
    spread,
    gather,
    outg,
    hist,
    far,
    send_a,
    send_b,
    send_c,
    recv_a,
    recv_b,
    recv_c,
    port_recv,
    load_sem,
    sems,
    psend,
    precv,
):
    sub = lax.axis_index("sub")
    me = lax.axis_index("split")
    sibling = me + 1 - 2 * lax.rem(me, 2)
    across = lax.rem(me + 2, 4)
    diagonal = lax.rem(sibling + 2, 4)
    cont = volt_ref.shape[1]
    nodes = volt_ref.shape[2]
    ports = hist0_ref.shape[2]
    stride = nodes // ports
    rows = cont // HALVES
    per = HALVES // GROUPS
    wide = cont // GROUPS
    packed, capacity, lanes = packing(n_subs, ports, cont)
    owners = (diagonal, across, sibling, me)

    strips = nodes // 128

    def load(slot, i):
        start = pl.multiple_of(owners[slot] * nodes, nodes)
        return pltpu.make_async_copy(
            inv_ref.at[0, pl.ds(start, nodes), pl.ds(i * 128, 128)],
            mat.at[i, pl.ds(slot * nodes, nodes), :],
            load_sem.at[slot, i],
        )

    for slot in range(4):
        for i in range(strips):
            load(slot, i).start()

    barrier = pltpu.get_barrier_semaphore()
    for other in (sibling, across):
        pl.semaphore_signal(barrier, inc=1, device_id=(sub, other), device_id_type=MESH)

    def each_peer(body):
        if n_subs <= 16:
            for j in range(1, n_subs):
                body(j)
        else:

            def step_of(j, c):
                body(j)
                return c

            lax.fori_loop(1, n_subs, step_of, 0)

    def greet(j):
        pl.semaphore_signal(
            barrier, inc=1, device_id=(lax.rem(sub + j, n_subs), me), device_id_type=MESH
        )

    each_peer(greet)

    line = lax.broadcasted_iota(jnp.int32, (nodes, nodes), 0)
    node = lax.broadcasted_iota(jnp.int32, (nodes, nodes), 1)
    wanted = (line % ports) * stride + line // ports
    perm[...] = jnp.where(node == wanted, 1.0, 0.0).astype(jnp.bfloat16)

    small = jnp.concatenate(
        [amp_ref[...], phase_ref[...], comp_ref[...], jnp.zeros((5, nodes), jnp.float32), volt_ref[0]], 0
    )
    small = exact_dot(small, perm[...], NT)
    amp, phase = small[0:1], small[1:2]
    when = (lax.broadcasted_iota(jnp.int32, (STEPS, nodes), 0) + 1).astype(jnp.float32)
    source = amp * jnp.cos(jnp.float32(angular) * when + phase)
    for step in range(STEPS):
        src[step] = source[step : step + 1]
    src[STEPS] = small[2:3]
    for half in range(HALVES):
        vol[half] = small[8 + half * rows : 8 + (half + 1) * rows]

    for group in range(GROUPS):
        for early in range(DMAX):
            far[early, group] = -hist0_ref[0, group * wide : (group + 1) * wide, :]

    partner = partner_ref[...]
    if packed:
        across_row = jnp.broadcast_to(partner.astype(jnp.float32), (ports, ports))
        down = across_row.T
        up = lax.broadcasted_iota(jnp.int32, (ports, ports), 0)
        right_of = lax.broadcasted_iota(jnp.int32, (ports, ports), 1)
        same = jnp.where(across_row == down, 1.0, 0.0)
        rank_row = jnp.sum(jnp.where(up < right_of, same, 0.0), axis=0, keepdims=True)
        rank_col = jnp.sum(jnp.where(right_of < up, same, 0.0), axis=1, keepdims=True)
        slot_row = across_row[:1] * capacity + rank_row
        slot_col = down * capacity + rank_col
        for q in range(n_subs):
            base = q * capacity
            want_col = (base + right_of % capacity).astype(jnp.float32)
            hit_col = jnp.where(slot_col == want_col, 1.0, 0.0)
            want_row = (base + up % capacity).astype(jnp.float32)
            hit_row = jnp.where(slot_row == want_row, 1.0, 0.0)
            for g in range(lanes):
                spread[g * ports : (g + 1) * ports, q * ports : (q + 1) * ports] = jnp.where(
                    right_of // capacity == g, hit_col, 0.0
                ).astype(jnp.bfloat16)
                gather[q * ports : (q + 1) * ports, g * ports : (g + 1) * ports] = jnp.where(
                    up // capacity == g, hit_row, 0.0
                ).astype(jnp.bfloat16)

    def prepare(slot, c):
        base = slot * nodes
        for j in range(stride):
            chunk = jnp.concatenate(
                [
                    mat[i, pl.ds(base + j, ports, stride=stride), :]
                    for i in range(strips)
                ],
                1,
            )
            top, rest = parts_of(chunk, 2)
            cols = pl.ds(j * ports, ports)
            high[slot, :, cols] = dot(perm[...], top, NT).astype(jnp.bfloat16)
            low[slot, :, cols] = dot(perm[...], rest, NT).astype(jnp.bfloat16)
        return c

    for slot in range(4):
        for i in range(strips):
            load(slot, i).wait()
        prepare(slot, 0)

    pl.semaphore_wait(barrier, n_subs + 1)

    def remote(kind, t, half):
        source_ref, target_ref, device = (
            (send_a, recv_a, sibling),
            (send_b, recv_b, sibling),
            (send_c, recv_c, across),
        )[kind]
        return pltpu.make_async_remote_copy(
            src_ref=source_ref.at[t, half],
            dst_ref=target_ref.at[t, half],
            send_sem=sems.at[0, kind, t, half],
            recv_sem=sems.at[1, kind, t, half],
            device_id=(sub, device),
            device_id_type=MESH,
        )

    impedance = surge_ref[...]
    delays = delay_ref[...]

    def all_ports(t, group, sem):
        return pltpu.make_async_copy(
            port_recv.at[t, group], port_recv.at[t, group], sem.at[t, group]
        )

    def opened(t, half):
        return t < open_ref[0, half * rows : (half + 1) * rows, :]

    def finish(t, half):
        remote(1, t, half).wait_recv()
        remote(2, t, half).wait_recv()
        done = kept[half] + recv_b[t, half] + recv_c[t, half]
        vol[half] = done
        return done

    def outgoing(t, half, done):
        ratio = done[:, :ports] / impedance
        within = half % per * rows
        value[half // per, within : within + rows] = jnp.where(
            opened(t, half), 2.0 * ratio + hist[half], 0.0
        )

    def ports_out(t, group):
        if packed:
            tall = value[group]
            high_rows = wide // lanes
            flat = jnp.concatenate(
                [tall[g * high_rows : (g + 1) * high_rows] for g in range(lanes)], 1
            )
            sent = exact_dot(flat, spread[...], NN)
            for q in range(n_subs):
                outg[t, group, q] = sent[:, q * ports : (q + 1) * ports]
        else:
            outg[t, group, 0] = value[group]

        def send(j):
            peer = lax.rem(sub + j, n_subs)
            pltpu.make_async_remote_copy(
                src_ref=outg.at[t, group, peer if packed else 0],
                dst_ref=port_recv.at[t, group, j - 1],
                send_sem=psend.at[t, group],
                recv_sem=precv.at[t, group],
                device_id=(peer, me),
                device_id_type=MESH,
            ).start()

        each_peer(send)

    def ports_in(t, group):
        all_ports(t, group, precv).wait()
        if packed:
            pieces = []
            for q in range(n_subs):
                j = lax.rem(sub + n_subs - q, n_subs)
                block = port_recv[t, group, jnp.maximum(j - 1, 0)]
                pieces.append(block)
            flat = exact_dot(jnp.concatenate(pieces, 1), gather[...], NN)
            total = jnp.concatenate(
                [flat[:, g * ports : (g + 1) * ports] for g in range(lanes)], 0
            )
        else:

            def pick(j, total):
                origin = lax.rem(sub + n_subs - j, n_subs)
                return jnp.where(partner == origin, port_recv[t, group, j - 1], total)

            total = jnp.zeros((wide, ports), jnp.float32)
            if n_subs <= 16:
                for j in range(1, n_subs):
                    total = pick(j, total)
            else:
                total = lax.fori_loop(1, n_subs, pick, total)
        far[t + DMAX, group] = total

    def begin(t, half):
        group, place = half // per, half % per
        within = slice(place * rows, (place + 1) * rows)

        @pl.when(t >= 1)
        def _():
            outgoing(t - 1, half, finish(t - 1, half))

        if place == 0:

            @pl.when(t >= DMIN)
            def _():
                ports_in(t - DMIN, group)

        history = jnp.zeros((rows, ports), jnp.float32)
        for d in range(DMIN, DMAX + 1):
            history = jnp.where(delays == d, -far[t - d + DMAX, group, within], history)
        hist[half] = history
        inject = jnp.where(opened(t, half), history, 0.0)
        right = src[t] + src[STEPS] * vol[half]
        right = jnp.concatenate([right[:, :ports] - inject, right[:, ports:]], 1)
        both = jnp.concatenate(parts_of(right, 2), 0)

        def product(slot):
            twice = dot(both, high[slot])
            return (twice[:rows] + twice[rows:]) + dot(both[:rows], low[slot])

        send_a[t, half] = product(0)
        remote(0, t, half).start()
        if place == per - 1:

            @pl.when((t >= 1) & (t - 1 + DMIN < STEPS))
            def _():
                ports_out(t - 1, group)

        send_b[t, half] = product(2)
        remote(1, t, half).start()
        mine[half] = product(1)
        kept[half] = product(3)

    def relay(t, half):
        remote(0, t, half).wait_recv()
        send_c[t, half] = mine[half] + recv_a[t, half]
        remote(2, t, half).start()

    def step_of(t, c):
        for turn in range(HALVES + LAG):
            if turn < HALVES:
                begin(t, turn)
            if turn >= LAG:
                relay(t, turn - LAG)
        return c

    lax.fori_loop(0, STEPS, step_of, 0)

    last = STEPS - 1
    for half in range(HALVES):
        done = finish(last, half)
        span = slice(half * rows, (half + 1) * rows)
        ratio = done[:, :ports] / impedance
        out_cur_ref[0, span, :] = jnp.where(opened(last, half), ratio + hist[half], 0.0)
        out_volt_ref[0, span, :] = exact_dot(done, perm[...], NN)

    def drain(t, c):
        for half in range(HALVES):
            for kind in range(3):
                remote(kind, t, half).wait_send()

        @pl.when(t + DMIN < STEPS)
        def _():
            for group in range(GROUPS):
                all_ports(t, group, psend).wait()

        return c

    lax.fori_loop(0, STEPS, drain, 0)


def local(*args):
    n_subs = lax.axis_size("sub")
    volt, hist0 = args[5], args[6]
    cont, nodes = volt.shape[1], volt.shape[2]
    ports = hist0.shape[2]
    rows = cont // HALVES
    f32, bf16 = jnp.float32, jnp.bfloat16
    block = (STEPS, HALVES, rows, nodes)
    vmem = pl.BlockSpec(memory_space=pltpu.VMEM)
    moves = STEPS - DMIN
    wide = cont // GROUPS
    packed, _, lanes = packing(n_subs, ports, cont)
    port_rows = wide // lanes if packed else wide
    blocks = n_subs if packed else 1
    dma = pltpu.SemaphoreType.DMA
    return pl.pallas_call(
        functools.partial(kernel, n_subs),
        out_shape=(
            jax.ShapeDtypeStruct(volt.shape, f32),
            jax.ShapeDtypeStruct(hist0.shape, f32),
        ),
        in_specs=[pl.BlockSpec(memory_space=pl.ANY)] + [vmem] * 9,
        out_specs=(vmem, vmem),
        scratch_shapes=[
            pltpu.VMEM((nodes // 128, 4 * nodes, 128), f32),
            pltpu.VMEM((4, nodes, nodes), bf16),
            pltpu.VMEM((4, nodes, nodes), bf16),
            pltpu.VMEM((nodes, nodes), bf16),
            pltpu.VMEM((HALVES, rows, nodes), f32),
            pltpu.VMEM((STEPS + 1, 1, nodes), f32),
            pltpu.VMEM((HALVES, rows, nodes), f32),
            pltpu.VMEM((HALVES, rows, nodes), f32),
            pltpu.VMEM((GROUPS, wide, ports), f32),
            pltpu.VMEM((lanes * ports, n_subs * ports) if packed else (16, 128), bf16),
            pltpu.VMEM((n_subs * ports, lanes * ports) if packed else (16, 128), bf16),
            pltpu.VMEM((moves, GROUPS, blocks, port_rows, ports), f32),
            pltpu.VMEM((HALVES, rows, ports), f32),
            pltpu.VMEM((STEPS + DMAX, GROUPS, wide, ports), f32),
            pltpu.VMEM(block, f32),
            pltpu.VMEM(block, f32),
            pltpu.VMEM(block, f32),
            pltpu.VMEM(block, f32),
            pltpu.VMEM(block, f32),
            pltpu.VMEM(block, f32),
            pltpu.VMEM((moves, GROUPS, n_subs - 1, port_rows, ports), f32),
            dma((4, nodes // 128)),
            dma((2, 3, STEPS, HALVES)),
            dma((moves, GROUPS)),
            dma((moves, GROUPS)),
        ],
        compiler_params=pltpu.CompilerParams(
            collective_id=0, has_side_effects=True, vmem_limit_bytes=62 * 1024 * 1024
        ),
    )(*args)


def solution(mesh):
    placed = (
        P("sub", None, "split"),
        P("sub", "split"),
        P("sub", "split"),
        P("sub", "split"),
        P("sub", "split"),
        P("sub", None, "split"),
        P("sub", None, "split"),
        P("sub", "split"),
        P("sub", "split"),
        P("sub", None, "split"),
    )
    return jax.shard_map(
        local,
        mesh=mesh,
        in_specs=placed,
        out_specs=(P("sub", None, "split"), P("sub", None, "split")),
        check_vma=False,
    )
```
